32 devices in a mesh: gz: 2 (over y), row: 4 (over z), col: 4 (over x, core).
Axes of the slice: x: 2, y: 2, z: 4, core: 2. Of those that a mesh axis runs over, the one named last changes fastest.
Arguments:
- lpanel: bfloat16 [2, 2, 1024, 2048], P(None, 'gz', 'row', 'col'), may hold values from -6 to 6
- upanel: bfloat16 [2, 2, 2048, 4096], P(None, 'gz', 'row', 'col'), may hold values from -0.125 to 0.125
- rowmap: int32 [2, 2, 4], P(None, 'gz', 'row'), may hold values from 0 to 1
- colmap: int32 [2, 2, 16], P(None, 'gz', 'col'), may hold values from 0 to 1
- blockmask: int32 [2, 2, 4, 16], P(None, 'gz', 'row', 'col'), may hold values 0 or 1
- front_blocks: bfloat16 [2, 2048, 2048], P(None, 'row', ('gz', 'col')), may hold values from -6 to 6
Outputs:
- front_update: bfloat16 [2, 2048, 2048], P(None, 'row', ('gz', 'col'))
The draws below stay inside these ranges and needn't reach their ends.
All inputs are finite; a program needn't handle non-finite values. No bound on the sum of `blockmask` on one device may be relied on, other than what follows from the above.
Results may differ from the reference program's by a relative error of at most 0.008.
Values may be sent and summed in bfloat16 or wider, within the bound.
No kernel may reach another device: no remote copies, remote signals or barrier semaphores. Data moves between devices by JAX's collectives and lax.ppermute only.
A program may use at most 64 MiB of HBM per device.

```python
import math
import jax
import jax.numpy as jnp
import numpy as np
from jax import lax

B = 256
W = 2048
CB = 4
FRB = 2
LEVELS = 2
UR = 1024
UC = 4096
FR = 2048
FC = 2048
N_GZ = 2
N_ROW = 4
N_COL = 4


def set_ends(values, rng, low, top_value):
    extent = values.shape
    place = [jax.random.randint(jax.random.fold_in(rng, axis), (), 0, extent[axis]) for axis in range(len(extent))]
    values = values.at[tuple(place)].set(low)
    longest = extent.index(max(extent))
    place[longest] = (place[longest] + 1) % extent[longest]
    return values.at[tuple(place)].set(top_value)


def level_of(rng, extent, cuts, least, top_value):
    gain = 1.0
    for position, blocks in cuts:
        draws = jax.random.uniform(jax.random.fold_in(jax.random.fold_in(rng, 6), position), (blocks,), jnp.float32, least / len(cuts), top_value / len(cuts))
        gain = gain * jnp.repeat(jnp.exp(draws), extent[position] // blocks).reshape((-1,) + (1,) * (len(extent) - 1 - position))
    return gain


def rank_bounds(amount, slope):
    portions = [(1 << 20) // math.isqrt(standing ** slope) + 1 for standing in range(1, amount + 1)]
    spread = 1 + sum(portions) // (1 << 30)
    return np.cumsum(np.array([max(1, weight // spread) for weight in portions]))


def ranked(own_key, extent, amount, slope):
    table = rank_bounds(amount, slope)
    pick = jax.random.randint(jax.random.fold_in(own_key, 1), extent, 0, int(table[amount - 1]))
    rank = jnp.searchsorted(jnp.asarray(table, jnp.int32), pick, side="right")
    return jax.random.permutation(jax.random.fold_in(own_key, 2), amount)[rank].astype(jnp.int32)


def gaussian(rng, shape, width, limit, pieces=(), kind=jnp.bfloat16):
    values = jax.random.normal(rng, shape, jnp.float32) * width
    if len(pieces) > 0:
        values = level_of(rng, shape, pieces, -0.22, 0.18) * values
    return jnp.clip(values, min=-limit, max=limit).astype(kind)


def setup_inputs(seed: int = 0) -> dict:
    key_list = jax.random.split(jax.random.key(seed), 7)
    lpanel = gaussian(key_list[0], (LEVELS, N_GZ, UR, W), 1.0, 6.0, ((1, 2), (2, 4), (3, 4)))
    upanel = gaussian(key_list[1], (LEVELS, N_GZ, W, UC), W ** -0.5, 0.125, ((1, 2), (2, 4), (3, 4)))
    rowmap = set_ends(jax.random.randint(key_list[2], (LEVELS, N_GZ, N_ROW), 0, FRB), jax.random.fold_in(key_list[2], 1), 0, FRB - 1).astype(jnp.int32)
    colmap = set_ends(ranked(key_list[3], (LEVELS, N_GZ, N_COL * CB), N_GZ, 2), jax.random.fold_in(key_list[3], 3), 0, N_GZ - 1).astype(jnp.int32)
    blockmask = set_ends((jax.random.randint(key_list[4], (LEVELS, N_GZ, N_ROW, N_COL * CB), 0, 4) < 3).astype(jnp.int32), jax.random.fold_in(key_list[4], 1), 0, 1)
    front_blocks = gaussian(key_list[5], (LEVELS, FR, FC), 1.0, 6.0, ((1, 4), (2, 8)))
    return dict(lpanel=lpanel, upanel=upanel, rowmap=rowmap, colmap=colmap, blockmask=blockmask, front_blocks=front_blocks)


def layer_partial(schur, rows_of, cols_of, live):
    blocks = schur.reshape(N_ROW, B, N_COL, CB, B)
    targets = cols_of.reshape(N_COL, CB)[:, :, None] == jnp.arange(N_GZ, dtype=jnp.int32)[None, None, :]
    col_select = targets.astype(jnp.float32)[None] * live.reshape(N_ROW, N_COL, CB).astype(jnp.float32)[:, :, :, None]
    col_sums = jnp.einsum("rbcjk,rcjl->rblck", blocks, col_select, precision=lax.Precision.HIGHEST)
    row_select = (rows_of[:, None] == jnp.arange(FRB, dtype=jnp.int32)[None, :]).astype(jnp.float32)
    placed = row_select[:, :, None, None, None, None] * col_sums[:, None]
    return placed.reshape(FR, FC)


def reference(lpanel, upanel, rowmap, colmap, blockmask, front_blocks):
    results = []
    for depth in range(LEVELS):
        total = jnp.zeros((FR, FC), jnp.float32)
        for layer in range(N_GZ):
            schur = jnp.dot(lpanel[depth, layer], upanel[depth, layer], preferred_element_type=jnp.float32)
            partial_value = layer_partial(schur, rowmap[depth, layer], colmap[depth, layer], blockmask[depth, layer])
            total = total + partial_value.astype(jnp.bfloat16).astype(jnp.float32)
        results.append((front_blocks[depth].astype(jnp.float32) - total).astype(jnp.bfloat16))
    return jnp.stack(results)
```

```python
import jax
import jax.numpy as jnp
from jax import lax
from jax.experimental import pallas as pl
from jax.experimental.pallas import tpu as pltpu
from jax.sharding import PartitionSpec as P


def product_kernel(picks, left, right, out):
    slot = pl.program_id(0)
    layers, width = out.shape[1], out.shape[3]
    count = right.shape[1] // width
    tile = jnp.dot(left[0], right[...], preferred_element_type=jnp.float32)
    for layer in range(layers):
        total = None
        for j in range(count):
            term = picks[(slot * count + j) * layers + layer] * tile[:, j * width : (j + 1) * width]
            total = term if total is None else total + term
        out[0, layer] = total.astype(out.dtype)


def products(picks, left, right, layers):
    slots, rows, depth = left.shape
    columns = right.shape[1]
    width = rows
    return pl.pallas_call(
        product_kernel,
        grid=(slots,),
        in_specs=[
            pl.BlockSpec(memory_space=pltpu.SMEM),
            pl.BlockSpec((1, rows, depth), lambda i: (i, 0, 0)),
            pl.BlockSpec((depth, columns), lambda i: (0, 0)),
        ],
        out_specs=pl.BlockSpec((1, layers, rows, width), lambda i: (i, 0, 0, 0)),
        out_shape=jax.ShapeDtypeStruct((slots, layers, rows, width), jnp.bfloat16),
        cost_estimate=pl.CostEstimate(
            flops=2 * slots * rows * depth * columns,
            bytes_accessed=2 * (left.size + right.size + slots * layers * rows * width),
            transcendentals=0,
        ),
    )(picks, left, right)


def on_device(lpanel, upanel, rowmap, colmap, blockmask, front_blocks):
    layers, n_row, n_col = (lax.axis_size(name) for name in ("gz", "row", "col"))
    levels, _, rows, _ = lpanel.shape
    depth = upanel.shape[2]
    count = colmap.shape[2]
    places = front_blocks.shape[1] // rows
    folds = n_row // n_col
    layer, row, col = (lax.axis_index(name) for name in ("gz", "row", "col"))
    fold = row % folds

    lefts = []
    for level in range(levels):
        pieces = []
        for turn in range(folds):
            pairs = []
            for a in range(n_row):
                for k in range(n_col):
                    target = k * folds + (a // n_col + turn) % folds
                    pairs.append((a * n_col + k, target * n_col + a % n_col))
            part = lpanel[level, 0]
            if folds > 1:
                part = lax.dynamic_slice_in_dim(part, ((row // n_col + turn) % folds) * depth, depth, 1)
            pieces.append(lax.ppermute(part, ("row", "col"), pairs))
        held = jnp.stack(pieces)
        step = n_col // 2
        while step >= 1:
            other = lax.ppermute(held, "col", [(i, i ^ step) for i in range(n_col)])
            held = jnp.concatenate([held, other])
            step //= 2
        lefts.append(held)
    flips = [0]
    step = n_col // 2
    while step >= 1:
        flips = flips + [flip ^ step for flip in flips]
        step //= 2
    slot_flip = jnp.asarray([flip for flip in flips for _ in range(folds)], jnp.int32)
    slot_turn = jnp.asarray([turn for _ in flips for turn in range(folds)], jnp.int32)
    slot_block = (col ^ slot_flip) + n_col * ((fold - slot_turn) % folds)
    position = jnp.asarray([flips.index(flip) for flip in range(n_col)], jnp.int32)

    def slot_of(block):
        return position[col ^ (block % n_col)] * folds + (fold - block // n_col) % folds

    small = jnp.concatenate([rowmap.reshape(-1), blockmask.reshape(-1)])
    small = lax.all_gather(small, ("gz", "row")).reshape(layers, n_row, -1)
    every_row = lax.dynamic_index_in_dim(small, row, 1, False)[:, :levels]
    masks = lax.dynamic_index_in_dim(small, layer, 0, False)[:, levels:].reshape(n_row, levels, count)
    masks = masks[slot_block]

    results = []
    for level in range(levels):
        goes = colmap[level, 0][:, None] == jnp.arange(layers, dtype=jnp.int32)[None, :]
        picks = masks[:, level, :, None].astype(jnp.float32) * goes.astype(jnp.float32)[None]
        sums = products(picks.reshape(-1), lefts[level], upanel[level, 0], layers)

        def term(block):
            block = jnp.clip(block, 0, n_row - 1)
            return lax.dynamic_index_in_dim(sums, slot_of(block), 0, False)

        up = down = None
        for stage in range(1, n_row):
            send_up = term(n_row - stage + row)
            send_down = term(stage - n_row + row)
            if stage > 1:
                send_up = (send_up.astype(jnp.float32) + up.astype(jnp.float32)).astype(jnp.bfloat16)
                send_down = (send_down.astype(jnp.float32) + down.astype(jnp.float32)).astype(jnp.bfloat16)
            up = lax.ppermute(send_up, "row", [(z, z + 1) for z in range(stage)])
            down = lax.ppermute(send_down, "row", [(n_row - 1 - z, n_row - 2 - z) for z in range(stage)])
        mine = term(row).astype(jnp.float32) + up.astype(jnp.float32) + down.astype(jnp.float32)
        mine = mine.astype(jnp.bfloat16)
        placed = jnp.zeros((places, rows, rows), jnp.float32)
        spots = jnp.arange(places, dtype=jnp.int32)
        for turn in range(layers):
            block = lax.dynamic_index_in_dim(mine, (layer + turn) % layers, 0, False)
            if turn:
                block = lax.ppermute(block, "gz", [(g, (g + turn) % layers) for g in range(layers)])
            spot = every_row[(layer - turn) % layers, level]
            placed = placed + jnp.where((spots == spot)[:, None, None], block.astype(jnp.float32)[None], 0.0)
        placed = placed.reshape(places * rows, rows)
        results.append((front_blocks[level].astype(jnp.float32) - placed).astype(jnp.bfloat16))
    return jnp.stack(results)


def solution(mesh):
    return jax.shard_map(
        on_device,
        mesh=mesh,
        in_specs=(
            P(None, "gz", "row", "col"),
            P(None, "gz", "row", "col"),
            P(None, "gz", "row"),
            P(None, "gz", "col"),
            P(None, "gz", "row", "col"),
            P(None, "row", ("gz", "col")),
        ),
        out_specs=P(None, "row", ("gz", "col")),
        check_vma=False,
    )
```

```python
import functools

import jax
import jax.numpy as jnp
from jax import lax
from jax.experimental import pallas as pl
from jax.experimental.pallas import tpu as pltpu
from jax.sharding import PartitionSpec as P


def product_kernel(level, turns, n_row, n_col, *refs):
    folds = n_row // n_col
    masks, colmap = refs[:n_row], refs[n_row]
    lefts, right = refs[n_row + 1 : 2 * n_row + 1], refs[2 * n_row + 1]
    outs, held = refs[2 * n_row + 2 : -1], refs[-1]
    g, z, c = (lax.axis_index(name) for name in ("gz", "row", "col"))
    for slot, left in enumerate(lefts):
        held[slot] = left[...]
    layers, _, width = outs[0].shape
    count = right.shape[3] // width
    for turn, out in zip(turns, outs):
        a = z ^ turn
        slot = (c ^ (a % n_col)) * folds + ((z % folds) ^ (a // n_col))
        tile = jnp.dot(held[slot], right[0, 0], preferred_element_type=jnp.float32)
        for u in range(layers):
            total = None
            for j in range(count):
                pick = jnp.where(colmap[level, 0, j] == (g ^ u), masks[turn][level, 0, 0, j], 0)
                term = pick.astype(jnp.float32) * tile[:, j * width : (j + 1) * width]
                total = term if total is None else total + term
            out[u] = total.astype(out.dtype)


def products(level, turns, masks, colmap, lefts, upanel, layers, n_row, n_col):
    rows, depth = lefts[0].shape
    columns = upanel.shape[3]
    whole = pl.BlockSpec(memory_space=pltpu.VMEM)
    room = 4 * (2 * n_row * rows * depth + depth * columns + 2 * len(turns) * layers * rows * rows) + (4 << 20)
    return pl.pallas_call(
        functools.partial(product_kernel, level, turns, n_row, n_col),
        grid=(1,),
        in_specs=[pl.BlockSpec(memory_space=pltpu.SMEM)] * (n_row + 1)
        + [whole] * n_row
        + [pl.BlockSpec((1, 1, depth, columns), lambda i: (level, 0, 0, 0))],
        out_specs=[whole] * len(turns),
        out_shape=[jax.ShapeDtypeStruct((layers, rows, rows), jnp.bfloat16)] * len(turns),
        scratch_shapes=[pltpu.VMEM((n_row, rows, depth), jnp.bfloat16)],
        compiler_params=pltpu.CompilerParams(vmem_limit_bytes=room),
        cost_estimate=pl.CostEstimate(
            flops=2 * len(turns) * rows * depth * columns,
            bytes_accessed=2 * (n_row * rows * depth + depth * columns + len(turns) * layers * rows * rows),
            transcendentals=0,
        ),
        name=f"product_{level}_{turns[0]}",
    )(*masks, colmap, *lefts, upanel)


def place_kernel(level, layers, counts, *refs):
    maps, front, out = refs[:layers], refs[layers], refs[-1]
    blocks = list(refs[layers + 1 : layers + 1 + sum(counts)])
    width = out.shape[2]
    totals = []
    for n in counts:
        total = None
        for _ in range(n):
            ref = blocks.pop(0)
            term = (ref[0] if len(ref.shape) == 3 else ref[...]).astype(jnp.float32)
            total = term if total is None else total + term
        totals.append(total)
    for f in range(out.shape[1] // width):
        span = slice(f * width, (f + 1) * width)
        moved = None
        for u in range(layers):
            here = (maps[u][level, 0, 0] == f).astype(jnp.float32)
            moved = here * totals[u] if moved is None else moved + here * totals[u]
        out[0, span] = (front[0, span].astype(jnp.float32) - moved).astype(out.dtype)


def place(level, maps, front, groups, before):
    layers = len(groups)
    counts = tuple(len(group) for group in groups)
    _, height, width = front.shape
    specs = [pl.BlockSpec(memory_space=pltpu.SMEM)] * layers
    specs.append(pl.BlockSpec((1, height, width), lambda i: (level, 0, 0)))
    blocks = [block for group in groups for block in group]
    for block in blocks:
        if block.ndim == 3:
            specs.append(pl.BlockSpec((1, *block.shape[1:]), lambda i: (0, 0, 0)))
        else:
            specs.append(pl.BlockSpec(memory_space=pltpu.VMEM))
    args = [*maps, front, *blocks]
    aliases = {}
    if before is not None:
        aliases = {len(args): 0}
        args.append(before)
        specs.append(pl.BlockSpec(memory_space=pl.ANY))
    return pl.pallas_call(
        functools.partial(place_kernel, level, layers, counts),
        grid=(1,),
        in_specs=specs,
        out_specs=pl.BlockSpec((1, height, width), lambda i: (level, 0, 0)),
        out_shape=jax.ShapeDtypeStruct(front.shape, front.dtype),
        input_output_aliases=aliases,
        compiler_params=pltpu.CompilerParams(vmem_limit_bytes=32 * height * width + (2 << 20)),
        cost_estimate=pl.CostEstimate(
            flops=2 * layers * height * width, bytes_accessed=8 * height * width, transcendentals=0
        ),
        name=f"place_{level}",
    )(*args)


def on_device(lpanel, upanel, rowmap, colmap, blockmask, front_blocks):
    layers, n_row, n_col = (lax.axis_size(name) for name in ("gz", "row", "col"))
    levels = lpanel.shape[0]
    depth = upanel.shape[2]
    folds = n_row // n_col
    row = lax.axis_index("row")

    lefts = []
    for level in range(levels):
        hop = (level % 2) * (n_col // 2)
        pieces = {}
        for turn in range(folds):
            part = lpanel[level, 0]
            if folds > 1:
                part = lax.dynamic_slice_in_dim(part, ((row // n_col) ^ turn) * depth, depth, 1)
            if hop:
                part = lax.ppermute(part, "col", [(k, k ^ hop) for k in range(n_col)])
            pairs = []
            for a in range(n_row):
                for k in range(n_col):
                    target = k * folds + ((a // n_col) ^ turn)
                    pairs.append((a * n_col + (k ^ hop), target * n_col + a % n_col))
            pieces[0, turn] = lax.ppermute(part, ("row", "col"), pairs)
        step = n_col // 2
        while step >= 1:
            swap = [(k, k ^ step) for k in range(n_col)]
            for (flip, turn), piece in list(pieces.items()):
                pieces[flip ^ step, turn] = lax.ppermute(piece, "col", swap)
            step //= 2
        lefts.append([pieces[flip, turn] for flip in range(n_col) for turn in range(folds)])

    masks = [blockmask]
    for turn in range(1, n_row):
        masks.append(lax.ppermute(blockmask, "row", [(z, z ^ turn) for z in range(n_row)]))
    maps = [rowmap]
    for u in range(1, layers):
        maps.append(lax.ppermute(rowmap, "gz", [(g, g ^ u) for g in range(layers)]))

    def total(blocks):
        return sum(block.astype(jnp.float32) for block in blocks).astype(jnp.bfloat16)

    result = None
    half = n_row // 2
    away = [turn for turn in reversed(range(n_row)) if turn % 2]
    stay = [turn for turn in reversed(range(n_row)) if not turn % 2]
    for level in range(levels):
        terms = {}
        for turns in (away, stay):
            made = products(level, turns, masks, colmap, lefts[level], upanel, layers, n_row, n_col)
            terms.update({turn: [block] for turn, block in zip(turns, made)})
        bit = 1
        while bit < half:
            swap = [(z, z ^ bit) for z in range(n_row)]
            for turn in reversed(range(0, n_row, bit)):
                if turn & bit:
                    terms[turn ^ bit].append(lax.ppermute(total(terms.pop(turn)), "row", swap))
            bit *= 2
        groups = [terms[0]]
        ends = [(g, z) for g in range(layers) for z in range(n_row)]
        for u in range(layers):
            far = [(g * n_row + z, (g ^ u) * n_row + (z ^ half)) for g, z in ends]
            block = lax.ppermute(total([term[u] for term in terms[half]]), ("gz", "row"), far)
            if u:
                swap = [(g, g ^ u) for g in range(layers)]
                near = lax.ppermute(total([term[u] for term in terms[0]]), "gz", swap)
                groups.append([near, block])
            else:
                groups[0] = [*groups[0], block]
        result = place(level, maps, front_blocks, groups, result)
    return result


def solution(mesh):
    return jax.shard_map(
        on_device,
        mesh=mesh,
        in_specs=(
            P(None, "gz", "row", "col"),
            P(None, "gz", "row", "col"),
            P(None, "gz", "row"),
            P(None, "gz", "col"),
            P(None, "gz", "row", "col"),
            P(None, "row", ("gz", "col")),
        ),
        out_specs=P(None, "row", ("gz", "col")),
        check_vma=False,
    )
```

```python
import functools

import jax
import jax.numpy as jnp
from jax import lax
from jax.experimental import pallas as pl
from jax.experimental.pallas import tpu as pltpu
from jax.sharding import PartitionSpec as P


def prepare_kernel(n_row, *refs):
    masks, colmap, panel = refs[:n_row], refs[n_row], refs[n_row + 1]
    picks, held, done = refs[n_row + 2 :]
    copy = pltpu.make_async_copy(panel, held, done)
    copy.start()
    g = lax.axis_index("gz")
    levels, _, count = colmap.shape
    layers = picks.shape[0] // (levels * n_row * count)
    at = 0
    for level in range(levels):
        for turn in range(n_row):
            for u in range(layers):
                for j in range(count):
                    pick = jnp.where(colmap[level, 0, j] == (g ^ u), masks[turn][level, 0, 0, j], 0)
                    picks[at] = pick.astype(jnp.float32)
                    at += 1
    copy.wait()


def prepare(masks, colmap, upanel, layers):
    n_row = len(masks)
    levels, _, count = colmap.shape
    smem = pl.BlockSpec(memory_space=pltpu.SMEM)
    return pl.pallas_call(
        functools.partial(prepare_kernel, n_row),
        in_specs=[smem] * (n_row + 1) + [pl.BlockSpec(memory_space=pl.ANY)],
        out_specs=[smem, pl.BlockSpec(memory_space=pl.ANY)],
        out_shape=[
            jax.ShapeDtypeStruct((levels * n_row * layers * count,), jnp.float32),
            jax.ShapeDtypeStruct(upanel.shape, upanel.dtype),
        ],
        scratch_shapes=[pltpu.SemaphoreType.DMA],
        compiler_params=pltpu.CompilerParams(vmem_limit_bytes=1 << 20),
        cost_estimate=pl.CostEstimate(flops=1 << 20, bytes_accessed=4 * upanel.size, transcendentals=0),
        name="prepare",
    )(*masks, colmap, upanel)


def product_kernel(level, turns, n_row, n_col, layers, picks, *refs):
    folds = n_row // n_col
    lefts, right, outs, held = refs[:n_row], refs[n_row], list(refs[n_row + 1 : -1]), refs[-1]
    z, c = lax.axis_index("row"), lax.axis_index("col")
    for slot, left in enumerate(lefts):
        held[slot] = left[...]
    width = outs[0].shape[-1]
    count = right.shape[3] // width
    for turn, whole in turns:
        parts = [outs[0].at[u] for u in range(layers)] if whole else outs[:layers]
        del outs[: 1 if whole else layers]
        a = z ^ turn
        slot = (c ^ (a % n_col)) * folds + ((z % folds) ^ (a // n_col))
        tile = jnp.dot(held[slot], right[0, 0], preferred_element_type=jnp.float32)
        for u in range(layers):
            total = None
            for j in range(count):
                pick = picks[((level * n_row + turn) * layers + u) * count + j]
                term = pick * tile[:, j * width : (j + 1) * width]
                total = term if total is None else total + term
            parts[u][...] = total.astype(jnp.bfloat16)


def products(level, turns, picks, lefts, upanel, layers, n_col):
    n_row = len(lefts)
    rows, depth = lefts[0].shape
    columns = upanel.shape[3]
    whole = pl.BlockSpec(memory_space=pltpu.VMEM)
    room = 4 * (2 * n_row * rows * depth + depth * columns + 2 * len(turns) * layers * rows * rows) + (4 << 20)
    shapes = []
    for _, joint in turns:
        shapes += [(layers, rows, rows)] if joint else [(rows, rows)] * layers
    call = pl.pallas_call(
        functools.partial(product_kernel, level, turns, n_row, n_col, layers),
        grid=(1,),
        in_specs=[pl.BlockSpec(memory_space=pltpu.SMEM)]
        + [whole] * n_row
        + [pl.BlockSpec((1, 1, depth, columns), lambda i: (level, 0, 0, 0))],
        out_specs=[whole] * len(shapes),
        out_shape=[jax.ShapeDtypeStruct(shape, jnp.bfloat16) for shape in shapes],
        scratch_shapes=[pltpu.VMEM((n_row, rows, depth), jnp.bfloat16)],
        compiler_params=pltpu.CompilerParams(vmem_limit_bytes=room),
        cost_estimate=pl.CostEstimate(
            flops=2 * len(turns) * rows * depth * columns,
            bytes_accessed=2 * (n_row * rows * depth + depth * columns + len(turns) * layers * rows * rows),
            transcendentals=0,
        ),
    )
    made = list(call(picks, *lefts, upanel))
    results = []
    for _, joint in turns:
        results.append(made.pop(0) if joint else [made.pop(0) for _ in range(layers)])
    return results


def place_kernel(level, layers, counts, *refs):
    maps, front, out = refs[:layers], refs[layers], refs[-1]
    blocks = list(refs[layers + 1 : layers + 1 + sum(counts)])
    width = out.shape[2]
    totals = []
    for n in counts:
        total = None
        for _ in range(n):
            ref = blocks.pop(0)
            term = ref[...].astype(jnp.float32)
            total = term if total is None else total + term
        totals.append(total)
    for f in range(out.shape[1] // width):
        span = slice(f * width, (f + 1) * width)
        moved = None
        for u in range(layers):
            here = (maps[u][level, 0, 0] == f).astype(jnp.float32)
            moved = here * totals[u] if moved is None else moved + here * totals[u]
        out[0, span] = (front[0, span].astype(jnp.float32) - moved).astype(out.dtype)


def place(level, maps, front, groups, before):
    layers = len(groups)
    counts = tuple(len(group) for group in groups)
    _, height, width = front.shape
    specs = [pl.BlockSpec(memory_space=pltpu.SMEM)] * layers
    specs.append(pl.BlockSpec((1, height, width), lambda i: (level, 0, 0)))
    blocks = [block for group in groups for block in group]
    specs += [pl.BlockSpec(memory_space=pltpu.VMEM)] * len(blocks)
    args = [*maps, front, *blocks]
    aliases = {}
    if before is not None:
        aliases = {len(args): 0}
        args.append(before)
        specs.append(pl.BlockSpec(memory_space=pl.ANY))
    return pl.pallas_call(
        functools.partial(place_kernel, level, layers, counts),
        grid=(1,),
        in_specs=specs,
        out_specs=pl.BlockSpec((1, height, width), lambda i: (level, 0, 0)),
        out_shape=jax.ShapeDtypeStruct(front.shape, front.dtype),
        input_output_aliases=aliases,
        compiler_params=pltpu.CompilerParams(vmem_limit_bytes=32 * height * width + (2 << 20)),
        cost_estimate=pl.CostEstimate(
            flops=2 * layers * height * width, bytes_accessed=8 * height * width, transcendentals=0
        ),
    )(*args)


def on_device(lpanel, upanel, rowmap, colmap, blockmask, front_blocks):
    layers, n_row, n_col = (lax.axis_size(name) for name in ("gz", "row", "col"))
    levels = lpanel.shape[0]
    depth = upanel.shape[2]
    folds = n_row // n_col
    row = lax.axis_index("row")

    masks = [blockmask]
    for turn in range(1, n_row):
        masks.append(lax.ppermute(blockmask, "row", [(z, z ^ turn) for z in range(n_row)]))
    maps = [rowmap]
    for u in range(1, layers):
        maps.append(lax.ppermute(rowmap, "gz", [(g, g ^ u) for g in range(layers)]))

    lefts = []
    for level in range(levels):
        pieces = {}
        for turn in range(folds):
            part = lpanel[level, 0]
            if folds > 1:
                part = lax.dynamic_slice_in_dim(part, ((row // n_col) ^ turn) * depth, depth, 1)
            hop = (level % 2) * (n_col // 2)
            if hop:
                part = lax.ppermute(part, "col", [(k, k ^ hop) for k in range(n_col)])
            pairs = []
            for a in range(n_row):
                for k in range(n_col):
                    target = k * folds + ((a // n_col) ^ turn)
                    pairs.append((a * n_col + (k ^ hop), target * n_col + a % n_col))
            pieces[0, turn] = lax.ppermute(part, ("row", "col"), pairs)
        step = n_col // 2
        while step >= 1:
            swap = [(k, k ^ step) for k in range(n_col)]
            for (flip, turn), piece in list(pieces.items()):
                pieces[flip ^ step, turn] = lax.ppermute(piece, "col", swap)
            step //= 2
        lefts.append([pieces[flip, turn] for flip in range(n_col) for turn in range(folds)])
    picks, held = prepare(masks, colmap, upanel, layers)

    def total(blocks):
        if len(blocks) == 1:
            return blocks[0]
        return sum(block.astype(jnp.float32) for block in blocks).astype(jnp.bfloat16)

    result = None
    half = n_row // 2
    away = [(turn, turn & (turn - 1) != 0) for turn in reversed(range(n_row)) if turn % 2]
    stay = [(turn, turn & (turn - 1) != 0 or turn == half) for turn in reversed(range(n_row)) if not turn % 2]
    stay[-1] = (0, False)
    ends = [(g, z) for g in range(layers) for z in range(n_row)]
    for level in range(levels):
        terms = {}
        for turns in (away, stay):
            made = products(level, turns, picks, lefts[level], held, layers, n_col)
            terms.update({turn: [block] for (turn, _), block in zip(turns, made)})
        groups = [[block] for block in terms.pop(0)[0]]
        for u in range(1, layers):
            swap = [(g, g ^ u) for g in range(layers)]
            groups[u] = [lax.ppermute(groups[u][0], "gz", swap)]
        bit = 1
        while bit < n_row:
            swap = [(z, z ^ bit) for z in range(n_row)]
            for turn in reversed(range(0, n_row, bit)):
                if turn & bit and turn != bit:
                    terms[turn ^ bit].append(lax.ppermute(total(terms.pop(turn)), "row", swap))
            last = terms.pop(bit)
            for u in range(layers):
                block = total([term[u] for term in last])
                pairs = [(g * n_row + z, (g ^ u) * n_row + (z ^ bit)) for g, z in ends]
                groups[u].append(lax.ppermute(block, ("gz", "row"), pairs))
            bit *= 2
        result = place(level, maps, front_blocks, groups, result)
    return result


def solution(mesh):
    return jax.shard_map(
        on_device,
        mesh=mesh,
        in_specs=(
            P(None, "gz", "row", "col"),
            P(None, "gz", "row", "col"),
            P(None, "gz", "row"),
            P(None, "gz", "col"),
            P(None, "gz", "row", "col"),
            P(None, "row", ("gz", "col")),
        ),
        out_specs=P(None, "row", ("gz", "col")),
        check_vma=False,
    )
```

```python
import functools

import jax
import jax.numpy as jnp
from jax import lax
from jax.experimental import pallas as pl
from jax.experimental.pallas import tpu as pltpu
from jax.sharding import PartitionSpec as P


def prepare_kernel(n_row, *refs):
    masks, colmap, panel = refs[:n_row], refs[n_row], refs[n_row + 1]
    picks, held, done = refs[n_row + 2 :]
    copy = pltpu.make_async_copy(panel, held, done)
    copy.start()
    g = lax.axis_index("gz")
    levels, _, count = colmap.shape
    layers = picks.shape[0] // (levels * n_row * count)
    at = 0
    for level in range(levels):
        for turn in range(n_row):
            for u in range(layers):
                for j in range(count):
                    pick = jnp.where(colmap[level, 0, j] == (g ^ u), masks[turn][level, 0, 0, j], 0)
                    picks[at] = pick.astype(jnp.float32)
                    at += 1
    copy.wait()


def prepare(masks, colmap, upanel, layers):
    n_row = len(masks)
    levels, _, count = colmap.shape
    smem = pl.BlockSpec(memory_space=pltpu.SMEM)
    return pl.pallas_call(
        functools.partial(prepare_kernel, n_row),
        in_specs=[smem] * (n_row + 1) + [pl.BlockSpec(memory_space=pl.ANY)],
        out_specs=[smem, pl.BlockSpec(memory_space=pl.ANY)],
        out_shape=[
            jax.ShapeDtypeStruct((levels * n_row * layers * count,), jnp.float32),
            jax.ShapeDtypeStruct(upanel.shape, upanel.dtype),
        ],
        scratch_shapes=[pltpu.SemaphoreType.DMA],
        compiler_params=pltpu.CompilerParams(vmem_limit_bytes=1 << 20),
        cost_estimate=pl.CostEstimate(flops=1 << 20, bytes_accessed=4 * upanel.size, transcendentals=0),
        name="prepare",
    )(*masks, colmap, upanel)


def product_kernel(level, turns, n_row, n_col, layers, picks, *refs):
    folds = n_row // n_col
    lefts, right, outs, held = refs[:n_row], refs[n_row], list(refs[n_row + 1 : -1]), refs[-1]
    z, c = lax.axis_index("row"), lax.axis_index("col")
    for slot, left in enumerate(lefts):
        held[slot] = left[...]
    width = outs[0].shape[-1]
    count = right.shape[3] // width
    for turn, whole in turns:
        parts = [outs[0].at[u] for u in range(layers)] if whole else outs[:layers]
        del outs[: 1 if whole else layers]
        a = z ^ turn
        slot = (c ^ (a % n_col)) * folds + ((z % folds) ^ (a // n_col))
        tile = jnp.dot(held[slot], right[0, 0], preferred_element_type=jnp.float32)
        for u in range(layers):
            total = None
            for j in range(count):
                pick = picks[((level * n_row + turn) * layers + u) * count + j]
                term = pick * tile[:, j * width : (j + 1) * width]
                total = term if total is None else total + term
            parts[u][...] = total.astype(jnp.bfloat16)


def products(level, turns, picks, lefts, upanel, layers, n_col):
    n_row = len(lefts)
    rows, depth = lefts[0].shape
    columns = upanel.shape[3]
    whole = pl.BlockSpec(memory_space=pltpu.VMEM)
    room = 4 * (2 * n_row * rows * depth + depth * columns + 2 * len(turns) * layers * rows * rows) + (4 << 20)
    shapes = []
    for _, joint in turns:
        shapes += [(layers, rows, rows)] if joint else [(rows, rows)] * layers
    call = pl.pallas_call(
        functools.partial(product_kernel, level, turns, n_row, n_col, layers),
        grid=(1,),
        in_specs=[pl.BlockSpec(memory_space=pltpu.SMEM)]
        + [whole] * n_row
        + [pl.BlockSpec((1, 1, depth, columns), lambda i: (level, 0, 0, 0))],
        out_specs=[whole] * len(shapes),
        out_shape=[jax.ShapeDtypeStruct(shape, jnp.bfloat16) for shape in shapes],
        scratch_shapes=[pltpu.VMEM((n_row, rows, depth), jnp.bfloat16)],
        compiler_params=pltpu.CompilerParams(vmem_limit_bytes=room),
        cost_estimate=pl.CostEstimate(
            flops=2 * len(turns) * rows * depth * columns,
            bytes_accessed=2 * (n_row * rows * depth + depth * columns + len(turns) * layers * rows * rows),
            transcendentals=0,
        ),
    )
    made = list(call(picks, *lefts, upanel))
    results = []
    for _, joint in turns:
        results.append(made.pop(0) if joint else [made.pop(0) for _ in range(layers)])
    return results


def place_kernel(level, layers, counts, *refs):
    maps, front, out = refs[:layers], refs[layers], refs[-1]
    blocks = list(refs[layers + 1 : layers + 1 + sum(counts)])
    width = out.shape[2]
    totals = []
    for n in counts:
        total = None
        for _ in range(n):
            ref = blocks.pop(0)
            term = ref[...].astype(jnp.float32)
            total = term if total is None else total + term
        totals.append(total)
    for f in range(out.shape[1] // width):
        span = slice(f * width, (f + 1) * width)
        moved = None
        for u in range(layers):
            here = (maps[u][level, 0, 0] == f).astype(jnp.float32)
            moved = here * totals[u] if moved is None else moved + here * totals[u]
        out[0, span] = (front[0, span].astype(jnp.float32) - moved).astype(out.dtype)


def place(level, maps, front, groups, before):
    layers = len(groups)
    counts = tuple(len(group) for group in groups)
    _, height, width = front.shape
    specs = [pl.BlockSpec(memory_space=pltpu.SMEM)] * layers
    specs.append(pl.BlockSpec((1, height, width), lambda i: (level, 0, 0)))
    blocks = [block for group in groups for block in group]
    specs += [pl.BlockSpec(memory_space=pltpu.VMEM)] * len(blocks)
    args = [*maps, front, *blocks]
    aliases = {}
    if before is not None:
        aliases = {len(args): 0}
        args.append(before)
        specs.append(pl.BlockSpec(memory_space=pl.ANY))
    return pl.pallas_call(
        functools.partial(place_kernel, level, layers, counts),
        grid=(1,),
        in_specs=specs,
        out_specs=pl.BlockSpec((1, height, width), lambda i: (level, 0, 0)),
        out_shape=jax.ShapeDtypeStruct(front.shape, front.dtype),
        input_output_aliases=aliases,
        compiler_params=pltpu.CompilerParams(vmem_limit_bytes=32 * height * width + (2 << 20)),
        cost_estimate=pl.CostEstimate(
            flops=2 * layers * height * width, bytes_accessed=8 * height * width, transcendentals=0
        ),
    )(*args)


def on_device(lpanel, upanel, rowmap, colmap, blockmask, front_blocks):
    layers, n_row, n_col = (lax.axis_size(name) for name in ("gz", "row", "col"))
    levels = lpanel.shape[0]
    depth = upanel.shape[2]
    folds = n_row // n_col
    row = lax.axis_index("row")

    masks = [blockmask]
    for turn in range(1, n_row):
        masks.append(lax.ppermute(blockmask, "row", [(z, z ^ turn) for z in range(n_row)]))
    maps = [rowmap]
    for u in range(1, layers):
        maps.append(lax.ppermute(rowmap, "gz", [(g, g ^ u) for g in range(layers)]))

    lefts = []
    for level in range(levels):
        pieces = {}
        for turn in range(folds):
            part = lpanel[level, 0]
            if folds > 1:
                part = lax.dynamic_slice_in_dim(part, ((row // n_col) ^ turn) * depth, depth, 1)
            hop = (level % 2) * (n_col // 2)
            if hop:
                part = lax.ppermute(part, "col", [(k, k ^ hop) for k in range(n_col)])
            pairs = []
            for a in range(n_row):
                for k in range(n_col):
                    target = k * folds + ((a // n_col) ^ turn)
                    pairs.append((a * n_col + (k ^ hop), target * n_col + a % n_col))
            pieces[0, turn] = lax.ppermute(part, ("row", "col"), pairs)
        step = n_col // 2
        while step >= 1:
            swap = [(k, k ^ step) for k in range(n_col)]
            for (flip, turn), piece in list(pieces.items()):
                pieces[flip ^ step, turn] = lax.ppermute(piece, "col", swap)
            step //= 2
        lefts.append([pieces[flip, turn] for flip in range(n_col) for turn in range(folds)])
    picks, held = prepare(masks, colmap, upanel, layers)

    def total(blocks):
        if len(blocks) == 1:
            return blocks[0]
        return sum(block.astype(jnp.float32) for block in blocks).astype(jnp.bfloat16)

    result = None
    away = [(turn, False) for turn in reversed(range(n_row)) if turn % 2]
    stay = [(turn, False) for turn in reversed(range(n_row)) if not turn % 2]
    ends = [(g, z) for g in range(layers) for z in range(n_row)]
    for level in range(levels):
        terms = {}
        for turns in (away, stay):
            made = products(level, turns, picks, lefts[level], held, layers, n_col)
            terms.update({turn: [block] for (turn, _), block in zip(turns, made)})
        groups = [[block] for block in terms.pop(0)[0]]
        for u in range(1, layers):
            swap = [(g, g ^ u) for g in range(layers)]
            groups[u] = [lax.ppermute(groups[u][0], "gz", swap)]
        bit = 1
        while bit < n_row:
            swap = [(z, z ^ bit) for z in range(n_row)]
            for turn in reversed(range(0, n_row, bit)):
                if turn & bit and turn != bit:
                    parts = terms.pop(turn)
                    got = {}
                    for u in reversed(range(layers)):
                        block = total([part[u] for part in parts])
                        got[u] = lax.ppermute(block, "row", swap)
                    terms[turn ^ bit].append([got[u] for u in range(layers)])
            last = terms.pop(bit)
            for u in range(layers):
                block = total([term[u] for term in last])
                pairs = [(g * n_row + z, (g ^ u) * n_row + (z ^ bit)) for g, z in ends]
                groups[u].append(lax.ppermute(block, ("gz", "row"), pairs))
            bit *= 2
        result = place(level, maps, front_blocks, groups, result)
    return result


def solution(mesh):
    return jax.shard_map(
        on_device,
        mesh=mesh,
        in_specs=(
            P(None, "gz", "row", "col"),
            P(None, "gz", "row", "col"),
            P(None, "gz", "row"),
            P(None, "gz", "col"),
            P(None, "gz", "row", "col"),
            P(None, "row", ("gz", "col")),
        ),
        out_specs=P(None, "row", ("gz", "col")),
        check_vma=False,
    )
```

```python
import functools

import jax
import jax.numpy as jnp
from jax import lax
from jax.experimental import pallas as pl
from jax.experimental.pallas import tpu as pltpu
from jax.sharding import PartitionSpec as P


def landing(n_col):
    return min(1, n_col - 1)


def prepare_kernel(n_row, *refs):
    masks, colmap, panel = refs[:n_row], refs[n_row], refs[n_row + 1]
    picks, held, done = refs[n_row + 2 :]
    copy = pltpu.make_async_copy(panel, held, done)
    copy.start()
    g = lax.axis_index("gz")
    levels, _, count = colmap.shape
    layers = picks.shape[0] // (levels * n_row * count)
    at = 0
    for level in range(levels):
        for turn in range(n_row):
            for u in range(layers):
                for j in range(count):
                    pick = jnp.where(colmap[level, 0, j] == (g ^ u), masks[turn][level, 0, 0, j], 0)
                    picks[at] = pick.astype(jnp.float32)
                    at += 1
    copy.wait()


def prepare(masks, colmap, upanel, layers):
    n_row = len(masks)
    levels, _, count = colmap.shape
    smem = pl.BlockSpec(memory_space=pltpu.SMEM)
    return pl.pallas_call(
        functools.partial(prepare_kernel, n_row),
        in_specs=[smem] * (n_row + 1) + [pl.BlockSpec(memory_space=pl.ANY)],
        out_specs=[smem, pl.BlockSpec(memory_space=pl.ANY)],
        out_shape=[
            jax.ShapeDtypeStruct((levels * n_row * layers * count,), jnp.float32),
            jax.ShapeDtypeStruct(upanel.shape, upanel.dtype),
        ],
        scratch_shapes=[pltpu.SemaphoreType.DMA],
        compiler_params=pltpu.CompilerParams(vmem_limit_bytes=1 << 20),
        cost_estimate=pl.CostEstimate(flops=1 << 20, bytes_accessed=4 * upanel.size, transcendentals=0),
        name="prepare",
    )(*masks, colmap, upanel)


def product_kernel(level, turns, n_row, n_col, layers, picks, *refs):
    folds = n_row // n_col
    lefts, right, outs, held = refs[:n_row], refs[n_row], list(refs[n_row + 1 : -1]), refs[-1]
    z, c = lax.axis_index("row"), lax.axis_index("col")
    for slot, left in enumerate(lefts):
        held[slot] = left[...]
    width = outs[0].shape[-1]
    count = right.shape[3] // width
    for turn, whole in turns:
        parts = [outs[0].at[u] for u in range(layers)] if whole else outs[:layers]
        del outs[: 1 if whole else layers]
        a = z ^ turn
        slot = (c ^ (a % n_col) ^ landing(n_col)) * folds + ((z % folds) ^ (a // n_col))
        tile = jnp.dot(held[slot], right[0, 0], preferred_element_type=jnp.float32)
        for u in range(layers):
            total = None
            for j in range(count):
                pick = picks[((level * n_row + turn) * layers + u) * count + j]
                term = pick * tile[:, j * width : (j + 1) * width]
                total = term if total is None else total + term
            parts[u][...] = total.astype(jnp.bfloat16)


def products(level, turns, picks, lefts, upanel, layers, n_col):
    n_row = len(lefts)
    rows, depth = lefts[0].shape
    columns = upanel.shape[3]
    whole = pl.BlockSpec(memory_space=pltpu.VMEM)
    room = 4 * (2 * n_row * rows * depth + depth * columns + 2 * len(turns) * layers * rows * rows) + (4 << 20)
    shapes = []
    for _, joint in turns:
        shapes += [(layers, rows, rows)] if joint else [(rows, rows)] * layers
    call = pl.pallas_call(
        functools.partial(product_kernel, level, turns, n_row, n_col, layers),
        grid=(1,),
        in_specs=[pl.BlockSpec(memory_space=pltpu.SMEM)]
        + [whole] * n_row
        + [pl.BlockSpec((1, 1, depth, columns), lambda i: (level, 0, 0, 0))],
        out_specs=[whole] * len(shapes),
        out_shape=[jax.ShapeDtypeStruct(shape, jnp.bfloat16) for shape in shapes],
        scratch_shapes=[pltpu.VMEM((n_row, rows, depth), jnp.bfloat16)],
        compiler_params=pltpu.CompilerParams(vmem_limit_bytes=room),
        cost_estimate=pl.CostEstimate(
            flops=2 * len(turns) * rows * depth * columns,
            bytes_accessed=2 * (n_row * rows * depth + depth * columns + len(turns) * layers * rows * rows),
            transcendentals=0,
        ),
    )
    made = list(call(picks, *lefts, upanel))
    results = []
    for _, joint in turns:
        results.append(made.pop(0) if joint else [made.pop(0) for _ in range(layers)])
    return results


def place_kernel(level, layers, counts, *refs):
    maps, front, out = refs[:layers], refs[layers], refs[-1]
    blocks = list(refs[layers + 1 : layers + 1 + sum(counts)])
    width = out.shape[2]
    totals = []
    for n in counts:
        total = None
        for _ in range(n):
            ref = blocks.pop(0)
            term = ref[...].astype(jnp.float32)
            total = term if total is None else total + term
        totals.append(total)
    for f in range(out.shape[1] // width):
        span = slice(f * width, (f + 1) * width)
        moved = None
        for u in range(layers):
            here = (maps[u][level, 0, 0] == f).astype(jnp.float32)
            moved = here * totals[u] if moved is None else moved + here * totals[u]
        out[0, span] = (front[0, span].astype(jnp.float32) - moved).astype(out.dtype)


def place(level, maps, front, groups, before):
    layers = len(groups)
    counts = tuple(len(group) for group in groups)
    _, height, width = front.shape
    specs = [pl.BlockSpec(memory_space=pltpu.SMEM)] * layers
    specs.append(pl.BlockSpec((1, height, width), lambda i: (level, 0, 0)))
    blocks = [block for group in groups for block in group]
    specs += [pl.BlockSpec(memory_space=pltpu.VMEM)] * len(blocks)
    args = [*maps, front, *blocks]
    aliases = {}
    if before is not None:
        aliases = {len(args): 0}
        args.append(before)
        specs.append(pl.BlockSpec(memory_space=pl.ANY))
    return pl.pallas_call(
        functools.partial(place_kernel, level, layers, counts),
        grid=(1,),
        in_specs=specs,
        out_specs=pl.BlockSpec((1, height, width), lambda i: (level, 0, 0)),
        out_shape=jax.ShapeDtypeStruct(front.shape, front.dtype),
        input_output_aliases=aliases,
        compiler_params=pltpu.CompilerParams(vmem_limit_bytes=32 * height * width + (2 << 20)),
        cost_estimate=pl.CostEstimate(
            flops=2 * layers * height * width, bytes_accessed=8 * height * width, transcendentals=0
        ),
    )(*args)


def on_device(lpanel, upanel, rowmap, colmap, blockmask, front_blocks):
    layers, n_row, n_col = (lax.axis_size(name) for name in ("gz", "row", "col"))
    levels = lpanel.shape[0]
    depth = upanel.shape[2]
    folds = n_row // n_col
    row = lax.axis_index("row")

    masks = [blockmask]
    for turn in range(1, n_row):
        masks.append(lax.ppermute(blockmask, "row", [(z, z ^ turn) for z in range(n_row)]))
    maps = [rowmap]
    for u in range(1, layers):
        maps.append(lax.ppermute(rowmap, "gz", [(g, g ^ u) for g in range(layers)]))

    lefts = []
    for level in range(levels):
        pieces = {}
        for turn in range(folds):
            part = lpanel[level, 0]
            if folds > 1:
                part = lax.dynamic_slice_in_dim(part, ((row // n_col) ^ turn) * depth, depth, 1)
            hop = (level % 2) * (n_col // 2)
            if hop:
                part = lax.ppermute(part, "col", [(k, k ^ hop) for k in range(n_col)])
            pairs = []
            for a in range(n_row):
                for k in range(n_col):
                    target = k * folds + ((a // n_col) ^ turn)
                    pairs.append((a * n_col + (k ^ hop), target * n_col + (a % n_col ^ landing(n_col))))
            pieces[0, turn] = lax.ppermute(part, ("row", "col"), pairs)
        step = n_col // 2
        while step >= 1:
            swap = [(k, k ^ step) for k in range(n_col)]
            for (flip, turn), piece in list(pieces.items()):
                pieces[flip ^ step, turn] = lax.ppermute(piece, "col", swap)
            step //= 2
        lefts.append([pieces[flip, turn] for flip in range(n_col) for turn in range(folds)])
    picks, held = prepare(masks, colmap, upanel, layers)

    def total(blocks):
        if len(blocks) == 1:
            return blocks[0]
        return sum(block.astype(jnp.float32) for block in blocks).astype(jnp.bfloat16)

    result = None
    away = [(turn, False) for turn in reversed(range(n_row)) if turn % 2]
    stay = [(turn, False) for turn in reversed(range(n_row)) if not turn % 2]
    ends = [(g, z) for g in range(layers) for z in range(n_row)]
    for level in range(levels):
        terms = {}
        for turns in (away, stay):
            made = products(level, turns, picks, lefts[level], held, layers, n_col)
            terms.update({turn: [block] for (turn, _), block in zip(turns, made)})
        groups = [[block] for block in terms.pop(0)[0]]
        for u in range(1, layers):
            swap = [(g, g ^ u) for g in range(layers)]
            groups[u] = [lax.ppermute(groups[u][0], "gz", swap)]
        bit = 1
        while bit < n_row:
            swap = [(z, z ^ bit) for z in range(n_row)]
            for turn in reversed(range(0, n_row, bit)):
                if turn & bit and turn != bit:
                    parts = terms.pop(turn)
                    got = {}
                    for u in reversed(range(layers)):
                        block = total([part[u] for part in parts])
                        got[u] = lax.ppermute(block, "row", swap)
                    terms[turn ^ bit].append([got[u] for u in range(layers)])
            last = terms.pop(bit)
            for u in range(layers):
                block = total([term[u] for term in last])
                pairs = [(g * n_row + z, (g ^ u) * n_row + (z ^ bit)) for g, z in ends]
                groups[u].append(lax.ppermute(block, ("gz", "row"), pairs))
            bit *= 2
        result = place(level, maps, front_blocks, groups, result)
    return result


def solution(mesh):
    return jax.shard_map(
        on_device,
        mesh=mesh,
        in_specs=(
            P(None, "gz", "row", "col"),
            P(None, "gz", "row", "col"),
            P(None, "gz", "row"),
            P(None, "gz", "col"),
            P(None, "gz", "row", "col"),
            P(None, "row", ("gz", "col")),
        ),
        out_specs=P(None, "row", ("gz", "col")),
        check_vma=False,
    )
```
